32 devices in a mesh: groups: 2 (over x), seq: 16 (over z, y, core).
Axes of the slice: x: 2, y: 2, z: 4, core: 2. Of those that a mesh axis runs over, the one named last changes fastest.
Arguments:
- prefill_keys: bfloat16 [128, 4096, 128], P(('groups', 'seq')), parts along dimension 0, may hold values from -4 to 4
- prefill_values: bfloat16 [128, 4096, 128], P(('groups', 'seq')), parts along dimension 0, may hold values from -6 to 6
- window_queries: bfloat16 [128, 8, 256, 128], P(('groups', 'seq')), parts along dimension 0, may hold values from -48 to 48
- step_queries: bfloat16 [128, 2, 8, 128], P('groups'), parts along dimension 0, may hold values from -48 to 48
- new_keys: bfloat16 [128, 2, 128], P('groups'), parts along dimension 0, may hold values from -24 to 24
- new_values: bfloat16 [128, 2, 128], P('groups'), parts along dimension 0, may hold values from -6 to 6
- lengths: int32 [16], P('groups'), parts along dimension 0, may hold values from 2048 to 4096
- keep_mask: int32 [16, 32], P('groups'), parts along dimension 0, may hold values from 0 to 1, as said below
Outputs:
- cache_keys: bfloat16 [128, 4096, 128], P('groups', 'seq'), parts along dimension 0
- cache_values: bfloat16 [128, 4096, 128], P('groups', 'seq'), parts along dimension 0
- attended: bfloat16 [128, 2, 8, 128], P('groups'), parts along dimension 0
- block_scores: float32 [128, 32], P('groups', 'seq'), parts along dimension 0
The draws below stay inside these ranges and needn't reach their ends.
There are 2 independent parts, one for each index of `groups`. The reference program is written for one: setup_inputs(seed, part) draws one part's arguments, and reference() takes and returns one part's arrays. A program takes and returns all parts, laid end to end along the dimension named above; each array names one. Nothing has to cross between parts.
Inputs may be any that keep to these rules, and one draw needn't show every extreme that they name: `keep_mask`: 1 keeps a block, 0 drops it; block 0 of every sequence is kept.
All inputs are finite; a program needn't handle non-finite values.
Results may differ from the reference program's by a relative error of at most 0.0055.
Values may be sent and summed in bfloat16 or wider, within the bound.
No kernel may reach another device: no remote copies, remote signals or barrier semaphores. Data moves between devices by JAX's collectives and lax.ppermute only.
A program may use at most 128 MiB of HBM per device.

```python
import math
import jax
import jax.numpy as jnp
from jax import lax

KVH = 8
GROUP = 8
HD = 128
SEQS = 8
BLOCK = 128
WIN = 256
STEPS = 2
PAIRS = 64
LEN = 4096
NBLK = 32


def first_keys(key):
    return jnp.clip(jax.random.normal(jax.random.fold_in(key, 12), (PAIRS, HD), jnp.float32), -4.0, 4.0)


def draw_prefill_keys(key, part):
    entries = jnp.clip(jax.random.normal(jax.random.fold_in(key, 11), (PAIRS, LEN, HD), jnp.float32), -4.0, 4.0)
    return entries.at[:, 0, :].set(first_keys(key)).astype(jnp.bfloat16)


def draw_window_queries(key, part):
    sample = 3.0 * jnp.clip(jax.random.normal(jax.random.fold_in(key, 21), (PAIRS, GROUP, WIN, HD), jnp.float32), -4.0, 4.0)
    return sample.astype(jnp.bfloat16)


def plain_steps(key):
    return 3.0 * jnp.clip(jax.random.normal(jax.random.fold_in(key, 31), (PAIRS, STEPS, GROUP, HD), jnp.float32), -4.0, 4.0)


def step_sample(key):
    sample = plain_steps(key)
    return sample


def draw_step_queries(key, part):
    return step_sample(key).astype(jnp.bfloat16)


def draw_new_keys(key, part):
    centre = jnp.mean(plain_steps(key)[:, :, 1:, :].astype(jnp.bfloat16).astype(jnp.float32), axis=2)
    extra = jnp.clip(jax.random.normal(jax.random.fold_in(key, 41), (PAIRS, STEPS, HD), jnp.float32), -4.0, 4.0)
    return (centre + extra).astype(jnp.bfloat16)


def draw_keep_mask(key, part):
    picked = jax.random.randint(jax.random.fold_in(key, 51), (SEQS, NBLK), 0, 4)
    return jnp.where(picked < 3, 1, 0).astype(jnp.int32).at[:, 0].set(1)


def plant(result, stream_key, low, largest):
    longest = result.shape.index(max(result.shape))
    spots = []
    for shift in (0, 1):
        where = [jax.random.randint(jax.random.fold_in(stream_key, axis), (), 0, length) for axis, length in enumerate(result.shape)]
        where[longest] = (where[longest] + shift) % result.shape[longest]
        spots.append(tuple(where))
    return result.at[spots[0]].set(low).at[spots[1]].set(largest)


def level_of(own_key, extent, cuts, smallest, high):
    loudness = 1.0
    for dim, blocks in cuts:
        draws = jax.random.uniform(jax.random.fold_in(jax.random.fold_in(own_key, 6), dim), (blocks,), jnp.float32, smallest / len(cuts), high / len(cuts))
        loudness = loudness * jnp.repeat(jnp.exp(draws), extent[dim] // blocks).reshape((-1,) + (1,) * (len(extent) - 1 - dim))
    return loudness


def noise(key, extent, deviation, reach, shards=(), held_as=jnp.bfloat16):
    factor_of = level_of(key, extent, shards, -0.22, 0.18) if shards else 1.0
    drawn = jax.random.normal(key, extent, jnp.float32) * deviation * factor_of
    return jnp.minimum(jnp.maximum(drawn, -reach), reach).astype(held_as)


def setup_inputs(seed: int = 0, part: int = 0) -> dict:
    splits = jax.random.split(jax.random.key(seed), 9)
    part_splits = jax.random.split(jax.random.fold_in(splits[8], part), 9)
    prefill_keys = draw_prefill_keys(jax.random.fold_in(jax.random.fold_in(splits[8], part), 71), part)
    prefill_values = noise(part_splits[1], (PAIRS, LEN, HD), 1.0, 6.0, ((0, 16),))
    window_queries = draw_window_queries(jax.random.fold_in(jax.random.fold_in(splits[8], part), 71), part)
    step_queries = draw_step_queries(jax.random.fold_in(jax.random.fold_in(splits[8], part), 71), part)
    new_keys = draw_new_keys(jax.random.fold_in(jax.random.fold_in(splits[8], part), 71), part)
    new_values = noise(part_splits[5], (PAIRS, STEPS, HD), 1.0, 6.0)
    lengths = plant(jax.random.randint(part_splits[6], (SEQS,), LEN // 2, LEN + 1), jax.random.fold_in(part_splits[6], 1), LEN // 2, LEN).astype(jnp.int32)
    keep_mask = draw_keep_mask(jax.random.fold_in(jax.random.fold_in(splits[8], part), 71), part)
    return dict(prefill_keys=prefill_keys, prefill_values=prefill_values, window_queries=window_queries, step_queries=step_queries, new_keys=new_keys, new_values=new_values, lengths=lengths, keep_mask=keep_mask)


def window_prior(prefill_keys, window_queries, lengths, keep_mask):
    scaling = 1.0 / math.sqrt(HD)
    kept_tokens = jnp.repeat(keep_mask, BLOCK, axis=1) > 0
    position = jnp.arange(LEN, dtype=jnp.int32)
    offsets = jnp.tile(jnp.arange(WIN, dtype=jnp.int32), GROUP)

    def one_pair(pair_id):
        seq_id = pair_id // KVH
        query_rows = window_queries[pair_id].reshape(GROUP * WIN, HD)
        scores = jnp.dot(query_rows, prefill_keys[pair_id].T, preferred_element_type=jnp.float32) * scaling
        query_pos = lengths[seq_id] - WIN + offsets
        visible = kept_tokens[seq_id][None, :] & (position[None, :] <= query_pos[:, None])
        scores = jnp.where(visible, scores, -jnp.inf)
        highest = lax.optimization_barrier(jnp.max(scores, axis=1, keepdims=True))
        weights = jnp.exp(scores - highest)
        probability = weights / lax.optimization_barrier(jnp.sum(weights, axis=1, keepdims=True))
        return lax.optimization_barrier(jnp.sum(probability, axis=0)).reshape(NBLK, BLOCK).sum(axis=1) / GROUP
    return lax.map(one_pair, jnp.arange(PAIRS, dtype=jnp.int32))

def reference(prefill_keys, prefill_values, window_queries, step_queries, new_keys, new_values, lengths, keep_mask):
    prior_mass = window_prior(prefill_keys, window_queries, lengths, keep_mask).astype(jnp.bfloat16)
    scaling = 1.0 / math.sqrt(HD)
    position = jnp.arange(LEN, dtype=jnp.int32)
    kept_tokens = jnp.repeat(keep_mask, BLOCK, axis=1) > 0
    seq_visible = kept_tokens & (position[None, :] < lengths[:, None])
    pair_seq = jnp.arange(PAIRS, dtype=jnp.int32) // KVH
    visible = seq_visible[pair_seq]
    query_rows = step_queries.astype(jnp.float32).reshape(PAIRS, STEPS * GROUP, HD)
    scores = jnp.einsum('pqd,ptd->pqt', query_rows, prefill_keys.astype(jnp.float32), precision=lax.Precision.HIGHEST) * scaling
    scores = jnp.where(visible[:, None, :], scores, -jnp.inf)
    own_scores = jnp.einsum('pqd,pjd->pqj', query_rows, new_keys.astype(jnp.float32), precision=lax.Precision.HIGHEST) * scaling
    row_step = jnp.arange(STEPS * GROUP, dtype=jnp.int32) // GROUP
    own_visible = jnp.arange(STEPS, dtype=jnp.int32)[None, :] <= row_step[:, None]
    own_scores = jnp.where(own_visible[None], own_scores, -jnp.inf)
    highest = jnp.maximum(lax.optimization_barrier(jnp.max(scores, axis=2)), lax.optimization_barrier(jnp.max(own_scores, axis=2)))
    weights = jnp.exp(scores - highest[:, :, None])
    own_weights = jnp.exp(own_scores - highest[:, :, None])
    total_mass = lax.optimization_barrier(jnp.sum(weights, axis=2)) + lax.optimization_barrier(jnp.sum(own_weights, axis=2))
    rounded = lax.optimization_barrier(weights.astype(jnp.bfloat16)).astype(jnp.float32)
    own_rounded = lax.optimization_barrier(own_weights.astype(jnp.bfloat16)).astype(jnp.float32)
    summed = jnp.einsum('pqt,ptd->pqd', rounded, prefill_values.astype(jnp.float32), precision=lax.Precision.HIGHEST)
    summed = summed + jnp.einsum('pqj,pjd->pqd', own_rounded, new_values.astype(jnp.float32), precision=lax.Precision.HIGHEST)
    attended = (summed / total_mass[:, :, None]).astype(jnp.bfloat16).reshape(PAIRS, STEPS, GROUP, HD)
    new_mass = lax.optimization_barrier(jnp.sum(weights / total_mass[:, :, None], axis=1)).reshape(PAIRS, NBLK, BLOCK).sum(axis=2) / GROUP
    block_scores = prior_mass.astype(jnp.float32) + new_mass
    return (prefill_keys, prefill_values, attended, block_scores)
```

```python
import functools
import math

import jax
import jax.numpy as jnp
from jax import lax
from jax.experimental import pallas as pl
from jax.experimental.pallas import tpu as pltpu
from jax.sharding import PartitionSpec as P

KVH = 8
GROUP = 8
BLOCK = 128
HIDDEN = -1e30
ROWS = 256
CHUNK = 512


def window_kernel(lengths_ref, query_ref, key_ref, bias_ref, ones_ref, sum_ref, score_ref, *, window_size):
    step = pl.program_id(1)
    token_count, head_width = key_ref.shape[1:]
    row_count = query_ref.shape[1]
    scaling = math.log2(math.e) / math.sqrt(head_width)
    query_rows = query_ref[0]
    row_offset = lax.broadcasted_iota(jnp.int32, (row_count, 1), 0) + step * row_count
    query_pos = lengths_ref[pl.program_id(0)] - window_size + row_offset % window_size
    position = lax.broadcasted_iota(jnp.int32, (1, CHUNK), 1)
    peak = jnp.full((row_count, BLOCK), HIDDEN, jnp.float32)
    for first in range(0, token_count, CHUNK):
        scores = lax.dot_general(
            query_rows,
            key_ref[0, first : first + CHUNK, :],
            (((1,), (1,)), ((), ())),
            preferred_element_type=jnp.float32,
        )
        scores = scores * scaling + bias_ref[0, :, first : first + CHUNK]
        scores = jnp.where(position <= query_pos - first, scores, HIDDEN)
        score_ref[:, first : first + CHUNK] = scores
        for lane in range(0, CHUNK, BLOCK):
            peak = jnp.maximum(peak, scores[:, lane : lane + BLOCK])
    highest = jnp.max(peak, axis=1, keepdims=True)
    masses = jnp.zeros((row_count, ones_ref.shape[1]), jnp.float32)
    for first in range(0, token_count, CHUNK):
        weights = jnp.exp2(score_ref[:, first : first + CHUNK] - highest).astype(jnp.bfloat16)
        masses = masses + jnp.dot(
            weights, ones_ref[first : first + CHUNK, :], preferred_element_type=jnp.float32
        )
    total = jnp.sum(masses, axis=1, keepdims=True)
    result = jnp.sum(masses / total, axis=0, keepdims=True)

    @pl.when(step == 0)
    def _():
        sum_ref[...] = jnp.zeros_like(sum_ref)

    sum_ref[0] = sum_ref[0] + result


def window_mass(prefill_keys, window_queries, lengths_here, kept_blocks):
    pair_count, token_count, head_width = prefill_keys.shape
    block_count = kept_blocks.shape[1]
    window_size = window_queries.shape[2]
    rows_pair = window_queries.shape[1] * window_size
    query_rows = window_queries.reshape(pair_count, rows_pair, head_width)
    bias = jnp.broadcast_to(
        jnp.where(kept_blocks > 0, 0.0, HIDDEN).astype(jnp.float32)[:, :, None],
        (pair_count, block_count, BLOCK),
    ).reshape(pair_count, 1, token_count)
    width = -(-block_count // BLOCK) * BLOCK
    ones = (
        jnp.arange(token_count, dtype=jnp.int32)[:, None] // BLOCK
        == jnp.arange(width, dtype=jnp.int32)[None, :]
    ).astype(jnp.bfloat16)
    sums = pl.pallas_call(
        functools.partial(window_kernel, window_size=window_size),
        grid_spec=pltpu.PrefetchScalarGridSpec(
            num_scalar_prefetch=1,
            grid=(pair_count, rows_pair // ROWS),
            in_specs=[
                pl.BlockSpec((1, ROWS, head_width), lambda p, s, _: (p, s, 0)),
                pl.BlockSpec((1, token_count, head_width), lambda p, s, _: (p, 0, 0)),
                pl.BlockSpec((1, 1, token_count), lambda p, s, _: (p, 0, 0)),
                pl.BlockSpec((token_count, width), lambda p, s, _: (0, 0)),
            ],
            out_specs=pl.BlockSpec((1, 1, width), lambda p, s, _: (p, 0, 0)),
            scratch_shapes=[pltpu.VMEM((ROWS, token_count), jnp.float32)],
        ),
        out_shape=jax.ShapeDtypeStruct((pair_count, 1, width), jnp.float32),
        compiler_params=pltpu.CompilerParams(dimension_semantics=("arbitrary", "arbitrary")),
        name="window_mass",
    )(lengths_here, query_rows, prefill_keys, bias, ones)
    return sums[:, 0, :block_count] / GROUP


def select_rows(small_table, seq_ids):
    matches = seq_ids[:, None] == jnp.arange(small_table.shape[0], dtype=jnp.int32)[None, :]
    return jnp.sum(jnp.where(matches[:, :, None], small_table[None, :, :], 0), axis=1)


def step_scores(cache_part, queries_here, new_here, seq_length, kept):
    pair_count, token_count, head_width = cache_part.shape
    step_count = queries_here.shape[1]
    group_size = queries_here.shape[2]
    query_rows = queries_here.reshape(pair_count, step_count * group_size, head_width)
    scaling = 1.0 / math.sqrt(head_width)
    scores = (
        jnp.einsum("pqd,ptd->pqt", query_rows, cache_part, preferred_element_type=jnp.float32)
        * scaling
    )
    block_count = token_count // BLOCK
    kept_blocks = kept > 0
    kept_tokens = jnp.broadcast_to(
        kept_blocks[:, :, None], (pair_count, block_count, BLOCK)
    ).reshape(pair_count, token_count)
    position = jnp.arange(token_count, dtype=jnp.int32)
    visible = kept_tokens & (position[None, :] < seq_length[:, None])
    scores = jnp.where(visible[:, None, :], scores, -jnp.inf)
    own_scores = (
        jnp.einsum("pqd,pjd->pqj", query_rows, new_here, preferred_element_type=jnp.float32)
        * scaling
    )
    row_step = jnp.arange(step_count * group_size, dtype=jnp.int32) // group_size
    own_visible = jnp.arange(step_count, dtype=jnp.int32)[None, :] <= row_step[:, None]
    own_scores = jnp.where(own_visible[None], own_scores, -jnp.inf)
    return (scores, own_scores)


def local_terms(scores, cache_vals, highest):
    weights = jnp.exp(scores - highest[:, :, None])
    total_mass = jnp.sum(weights, axis=2)
    summed = jnp.einsum(
        "pqt,ptd->pqd", weights.astype(jnp.bfloat16), cache_vals, preferred_element_type=jnp.float32
    )
    return (weights, total_mass, summed)


def finish(summed, total_mass, weights, highest, own_scores, new_vals):
    own_weights = jnp.exp(own_scores - highest[:, :, None])
    total_mass = total_mass + jnp.sum(own_weights, axis=2)
    summed = summed + jnp.einsum(
        "pqj,pjd->pqd",
        own_weights.astype(jnp.bfloat16),
        new_vals,
        preferred_element_type=jnp.float32,
    )
    pair_count, row_count, head_width = summed.shape
    attended = (
        (summed / total_mass[:, :, None])
        .astype(jnp.bfloat16)
        .reshape(pair_count, row_count // GROUP, GROUP, head_width)
    )
    token_count = weights.shape[2]
    new_mass = (
        jnp.sum(weights / total_mass[:, :, None], axis=1)
        .reshape(pair_count, token_count // BLOCK, BLOCK)
        .sum(axis=2)
        / GROUP
    )
    return (attended, new_mass)


def local(
    prefill_keys,
    prefill_values,
    window_queries,
    step_queries,
    new_keys,
    new_values,
    lengths,
    keep_mask,
):
    pair_count, token_count, head_width = prefill_keys.shape
    place = lax.axis_index("seq")
    first_pair = place * pair_count
    seq_ids = (first_pair + jnp.arange(pair_count, dtype=jnp.int32)) // KVH
    kept = select_rows(keep_mask, seq_ids)
    seq_length = select_rows(lengths[:, None], seq_ids)[:, 0]

    device_count = lax.axis_size("seq")
    width = token_count // device_count

    def by_target(cache):
        blocks = cache.reshape(pair_count, device_count, width, head_width).transpose(1, 0, 2, 3)
        return blocks.reshape(device_count, pair_count * width, head_width)

    def exchange(blocks):
        moved = lax.all_to_all(blocks, "seq", split_axis=0, concat_axis=0, tiled=True)
        return moved.reshape(device_count * pair_count, width, head_width)

    cache_keys = exchange(by_target(prefill_keys))
    prior_mass = window_mass(prefill_keys, window_queries, seq_length, kept).astype(jnp.bfloat16)
    value_blocks, prior_mass, cache_keys = lax.optimization_barrier(
        (by_target(prefill_values), prior_mass, cache_keys)
    )
    cache_values = exchange(value_blocks)
    queries_here = lax.dynamic_slice_in_dim(step_queries, first_pair, pair_count, 0)
    new_keys_here = lax.dynamic_slice_in_dim(new_keys, first_pair, pair_count, 0)
    new_values_here = lax.dynamic_slice_in_dim(new_values, first_pair, pair_count, 0)
    scores, own_scores = step_scores(prefill_keys, queries_here, new_keys_here, seq_length, kept)
    highest = jnp.maximum(jnp.max(scores, axis=2), jnp.max(own_scores, axis=2))
    weights, total_mass, summed = local_terms(scores, prefill_values, highest)
    attended_here, mass_here = finish(
        summed, total_mass, weights, highest, own_scores, new_values_here
    )
    attended = lax.all_gather(attended_here, "seq", axis=0, tiled=True)
    block_mass = prior_mass.astype(jnp.float32) + mass_here
    block_scores = lax.all_to_all(block_mass, "seq", split_axis=1, concat_axis=0, tiled=True)
    return (cache_keys, cache_values, attended, block_scores)


def solution(mesh):
    placed = (
        P(("groups", "seq"), None, None),
        P(("groups", "seq"), None, None),
        P(("groups", "seq"), None, None, None),
        P("groups", None, None, None),
        P("groups", None, None),
        P("groups", None, None),
        P("groups"),
        P("groups", None),
    )
    return jax.shard_map(
        local,
        mesh=mesh,
        in_specs=placed,
        out_specs=(
            P("groups", "seq", None),
            P("groups", "seq", None),
            P("groups", None, None, None),
            P("groups", "seq"),
        ),
        check_vma=False,
    )
```

```python
import functools
import math

import jax
import jax.numpy as jnp
from jax import lax
from jax.experimental import pallas as pl
from jax.experimental.pallas import tpu as pltpu
from jax.sharding import PartitionSpec as P

KVH = 8
GROUP = 8
BLOCK = 128
HIDDEN = -1e30
ROWS = 256
CHUNK = 512
EARLY = 3
LATE = 3


def window_kernel(lengths_ref, query_ref, key_ref, bias_ref, ones_ref, sum_ref, score_ref, *, window_size):
    step = pl.program_id(1)
    token_count, head_width = key_ref.shape[1:]
    row_count = query_ref.shape[1]
    scaling = math.log2(math.e) / math.sqrt(head_width)
    query_rows = query_ref[0]
    row_offset = lax.broadcasted_iota(jnp.int32, (row_count, 1), 0) + step * row_count
    query_pos = lengths_ref[pl.program_id(0)] - window_size + row_offset % window_size
    position = lax.broadcasted_iota(jnp.int32, (1, CHUNK), 1)
    peak = jnp.full((row_count, BLOCK), HIDDEN, jnp.float32)
    for first in range(0, token_count, CHUNK):
        scores = lax.dot_general(
            query_rows,
            key_ref[0, first : first + CHUNK, :],
            (((1,), (1,)), ((), ())),
            preferred_element_type=jnp.float32,
        )
        scores = scores * scaling + bias_ref[0, :, first : first + CHUNK]
        scores = jnp.where(position <= query_pos - first, scores, HIDDEN)
        score_ref[:, first : first + CHUNK] = scores
        for lane in range(0, CHUNK, BLOCK):
            peak = jnp.maximum(peak, scores[:, lane : lane + BLOCK])
    highest = jnp.max(peak, axis=1, keepdims=True)
    masses = jnp.zeros((row_count, ones_ref.shape[1]), jnp.float32)
    for first in range(0, token_count, CHUNK):
        weights = jnp.exp2(score_ref[:, first : first + CHUNK] - highest).astype(jnp.bfloat16)
        masses = masses + jnp.dot(
            weights, ones_ref[first : first + CHUNK, :], preferred_element_type=jnp.float32
        )
    total = jnp.sum(masses, axis=1, keepdims=True)
    result = jnp.sum(masses / total, axis=0, keepdims=True)

    @pl.when(step == 0)
    def _():
        sum_ref[...] = jnp.zeros_like(sum_ref)

    sum_ref[0] = sum_ref[0] + result


def window_mass(prefill_keys, window_queries, lengths_here, kept_blocks):
    pair_count, token_count, head_width = prefill_keys.shape
    block_count = kept_blocks.shape[1]
    window_size = window_queries.shape[2]
    rows_pair = window_queries.shape[1] * window_size
    query_rows = window_queries.reshape(pair_count, rows_pair, head_width)
    bias = jnp.broadcast_to(
        jnp.where(kept_blocks > 0, 0.0, HIDDEN).astype(jnp.float32)[:, :, None],
        (pair_count, block_count, BLOCK),
    ).reshape(pair_count, 1, token_count)
    width = -(-block_count // BLOCK) * BLOCK
    ones = (
        jnp.arange(token_count, dtype=jnp.int32)[:, None] // BLOCK
        == jnp.arange(width, dtype=jnp.int32)[None, :]
    ).astype(jnp.bfloat16)
    sums = pl.pallas_call(
        functools.partial(window_kernel, window_size=window_size),
        grid_spec=pltpu.PrefetchScalarGridSpec(
            num_scalar_prefetch=1,
            grid=(pair_count, rows_pair // ROWS),
            in_specs=[
                pl.BlockSpec((1, ROWS, head_width), lambda p, s, _: (p, s, 0)),
                pl.BlockSpec((1, token_count, head_width), lambda p, s, _: (p, 0, 0)),
                pl.BlockSpec((1, 1, token_count), lambda p, s, _: (p, 0, 0)),
                pl.BlockSpec((token_count, width), lambda p, s, _: (0, 0)),
            ],
            out_specs=pl.BlockSpec((1, 1, width), lambda p, s, _: (p, 0, 0)),
            scratch_shapes=[pltpu.VMEM((ROWS, token_count), jnp.float32)],
        ),
        out_shape=jax.ShapeDtypeStruct((pair_count, 1, width), jnp.float32),
        compiler_params=pltpu.CompilerParams(dimension_semantics=("arbitrary", "arbitrary")),
        name="window_mass",
    )(lengths_here, query_rows, prefill_keys, bias, ones)
    return sums[:, 0, :block_count] / GROUP


def select_rows(small_table, seq_ids):
    matches = seq_ids[:, None] == jnp.arange(small_table.shape[0], dtype=jnp.int32)[None, :]
    return jnp.sum(jnp.where(matches[:, :, None], small_table[None, :, :], 0), axis=1)


def step_scores(cache_part, queries_here, new_here, seq_length, kept):
    pair_count, token_count, head_width = cache_part.shape
    step_count = queries_here.shape[1]
    group_size = queries_here.shape[2]
    query_rows = queries_here.reshape(pair_count, step_count * group_size, head_width)
    scaling = 1.0 / math.sqrt(head_width)
    scores = (
        jnp.einsum("pqd,ptd->pqt", query_rows, cache_part, preferred_element_type=jnp.float32)
        * scaling
    )
    block_count = token_count // BLOCK
    kept_blocks = kept > 0
    kept_tokens = jnp.broadcast_to(
        kept_blocks[:, :, None], (pair_count, block_count, BLOCK)
    ).reshape(pair_count, token_count)
    position = jnp.arange(token_count, dtype=jnp.int32)
    visible = kept_tokens & (position[None, :] < seq_length[:, None])
    scores = jnp.where(visible[:, None, :], scores, -jnp.inf)
    own_scores = (
        jnp.einsum("pqd,pjd->pqj", query_rows, new_here, preferred_element_type=jnp.float32)
        * scaling
    )
    row_step = jnp.arange(step_count * group_size, dtype=jnp.int32) // group_size
    own_visible = jnp.arange(step_count, dtype=jnp.int32)[None, :] <= row_step[:, None]
    own_scores = jnp.where(own_visible[None], own_scores, -jnp.inf)
    return (scores, own_scores)


def local_terms(scores, cache_vals, highest):
    weights = jnp.exp(scores - highest[:, :, None])
    total_mass = jnp.sum(weights, axis=2)
    summed = jnp.einsum(
        "pqt,ptd->pqd", weights.astype(jnp.bfloat16), cache_vals, preferred_element_type=jnp.float32
    )
    return (weights, total_mass, summed)


def finish(summed, total_mass, weights, highest, own_scores, new_vals):
    own_weights = jnp.exp(own_scores - highest[:, :, None])
    total_mass = total_mass + jnp.sum(own_weights, axis=2)
    summed = summed + jnp.einsum(
        "pqj,pjd->pqd",
        own_weights.astype(jnp.bfloat16),
        new_vals,
        preferred_element_type=jnp.float32,
    )
    pair_count, row_count, head_width = summed.shape
    attended = (
        (summed / total_mass[:, :, None])
        .astype(jnp.bfloat16)
        .reshape(pair_count, row_count // GROUP, GROUP, head_width)
    )
    token_count = weights.shape[2]
    new_mass = (
        jnp.sum(weights / total_mass[:, :, None], axis=1)
        .reshape(pair_count, token_count // BLOCK, BLOCK)
        .sum(axis=2)
        / GROUP
    )
    return (attended, new_mass)


def cut_kernel(place_ref, cache_ref, *refs, partners, width):
    sems = refs[-1]
    copies = []
    for k, target in enumerate(partners(place_ref[0])):
        copies.append(
            pltpu.make_async_copy(
                cache_ref.at[:, pl.ds(target * width, width), :], refs[k], sems.at[k]
            )
        )
    for copy in copies:
        copy.start()
    for copy in copies:
        copy.wait()


def cut_blocks(place, cache, steps, partner, width):
    pair_count, _, head_width = cache.shape
    block = jax.ShapeDtypeStruct((pair_count, width, head_width), cache.dtype)
    return pl.pallas_call(
        functools.partial(
            cut_kernel, partners=lambda own: [partner(own, d)[0] for d in steps], width=width
        ),
        in_specs=[pl.BlockSpec(memory_space=pltpu.SMEM), pl.BlockSpec(memory_space=pl.ANY)],
        out_specs=[pl.BlockSpec(memory_space=pl.ANY)] * len(steps),
        out_shape=[block] * len(steps),
        scratch_shapes=[pltpu.SemaphoreType.DMA((len(steps),))],
        name="cut_blocks",
    )(place, cache)


def place_kernel(place_ref, whole_ref, *refs, sources, width, fresh):
    blocks, out_ref, sems = refs[:-2], refs[-2], refs[-1]
    own = place_ref[0]
    pair_count = blocks[0].shape[0]
    copies = [
        pltpu.make_async_copy(
            block, out_ref.at[pl.ds(source * pair_count, pair_count)], sems.at[k]
        )
        for k, (block, source) in enumerate(zip(blocks, sources(own)))
    ]
    if fresh:
        copies.append(
            pltpu.make_async_copy(
                whole_ref.at[:, pl.ds(own * width, width), :],
                out_ref.at[pl.ds(own * pair_count, pair_count)],
                sems.at[len(blocks)],
            )
        )
    for copy in copies:
        copy.start()
    for copy in copies:
        copy.wait()


def place_blocks(place, whole, blocks, steps, partner, device_count, fresh):
    pair_count, width, head_width = blocks[0].shape
    return pl.pallas_call(
        functools.partial(
            place_kernel,
            sources=lambda own: [partner(own, d)[1] for d in steps],
            width=width,
            fresh=fresh,
        ),
        in_specs=[pl.BlockSpec(memory_space=pltpu.SMEM)]
        + [pl.BlockSpec(memory_space=pl.ANY)] * (1 + len(blocks)),
        out_specs=pl.BlockSpec(memory_space=pl.ANY),
        out_shape=jax.ShapeDtypeStruct((device_count * pair_count, width, head_width), whole.dtype),
        scratch_shapes=[pltpu.SemaphoreType.DMA((len(blocks) + 1,))],
        input_output_aliases={} if fresh else {1: 0},
        name="place_blocks" if fresh else "place_last_blocks",
    )(place, whole, *blocks)


def local(
    prefill_keys,
    prefill_values,
    window_queries,
    step_queries,
    new_keys,
    new_values,
    lengths,
    keep_mask,
):
    pair_count, token_count, head_width = prefill_keys.shape
    place = lax.axis_index("seq")
    first_pair = place * pair_count
    seq_ids = (first_pair + jnp.arange(pair_count, dtype=jnp.int32)) // KVH

    device_count = lax.axis_size("seq")
    width = token_count // device_count
    half = device_count // 2
    steps = [half]
    for near in range(1, device_count - half):
        steps.append(near)
        if half + near < device_count:
            steps.append(half + near)
    paired = device_count & (device_count - 1) == 0

    def partner(own, d):
        if paired:
            return own ^ d, own ^ d
        return (own + d) % device_count, (own + device_count - d) % device_count

    def send(block, d):
        pairs = [(s, partner(s, d)[0]) for s in range(device_count)]
        return lax.ppermute(block, "seq", pairs)

    place_1 = place.reshape(1).astype(jnp.int32)
    early, later = steps[:EARLY], steps[EARLY:]
    first_blocks = cut_blocks(place_1, prefill_keys, early, partner, width)
    key_blocks = [send(b, d) for b, d in zip(first_blocks, early)]
    place_2, _ = lax.optimization_barrier((place_1, tuple(first_blocks)))
    more_blocks = cut_blocks(place_2, prefill_keys, later, partner, width)
    key_blocks += [send(b, d) for b, d in zip(more_blocks, later)]
    place_3, _ = lax.optimization_barrier((place_2, tuple(more_blocks)))
    value_cuts = cut_blocks(place_3, prefill_values, steps, partner, width)
    value_blocks = [send(b, d) for b, d in zip(value_cuts, steps)]
    place_4, _ = lax.optimization_barrier((place_3, tuple(value_cuts)))

    seq_ids = (place_4 * pair_count + jnp.arange(pair_count, dtype=jnp.int32)) // KVH
    first_pair = place_4[0] * pair_count
    kept = select_rows(keep_mask, seq_ids)
    seq_length = select_rows(lengths[:, None], seq_ids)[:, 0]
    prior_mass = window_mass(prefill_keys, window_queries, seq_length, kept).astype(jnp.bfloat16)
    queries_here = lax.dynamic_slice_in_dim(step_queries, first_pair, pair_count, 0)
    new_keys_here = lax.dynamic_slice_in_dim(new_keys, first_pair, pair_count, 0)
    new_values_here = lax.dynamic_slice_in_dim(new_values, first_pair, pair_count, 0)
    scores, own_scores = step_scores(prefill_keys, queries_here, new_keys_here, seq_length, kept)
    highest = jnp.maximum(jnp.max(scores, axis=2), jnp.max(own_scores, axis=2))
    weights, total_mass, summed = local_terms(scores, prefill_values, highest)
    attended_here, mass_here = finish(
        summed, total_mass, weights, highest, own_scores, new_values_here
    )
    block_mass = prior_mass.astype(jnp.float32) + mass_here
    high = lax.reduce_precision(block_mass, 8, 7)
    middle = lax.reduce_precision(block_mass - high, 8, 7)
    low = block_mass - high - middle
    mass_rows = jnp.concatenate([high, middle, low], axis=1).astype(jnp.bfloat16)
    mass_rows = jnp.pad(mass_rows, ((0, 0), (0, -mass_rows.shape[1] % head_width)))
    small = jnp.concatenate(
        [
            attended_here.reshape(pair_count, -1, head_width),
            mass_rows.reshape(pair_count, -1, head_width),
        ],
        axis=1,
    )

    place_5, small = lax.optimization_barrier((place_4, small))
    cache_keys = place_blocks(
        place_5, prefill_keys, key_blocks, steps, partner, device_count, True
    )
    place_6, cache_keys = lax.optimization_barrier((place_5, cache_keys))
    split = len(steps) - LATE
    partial_values = place_blocks(
        place_6, prefill_values, value_blocks[:split], steps[:split], partner, device_count, True
    )
    small, partial_values = lax.optimization_barrier((small, partial_values))
    gathered = lax.all_gather(small, "seq", axis=0, tiled=True)
    place_7, gathered = lax.optimization_barrier((place_6, gathered))
    cache_values = place_blocks(
        place_7, partial_values, value_blocks[split:], steps[split:], partner, device_count, False
    )
    step_count, group_size = step_queries.shape[1:3]
    rows = step_count * group_size
    attended = gathered[:, :rows].reshape(step_queries.shape)
    block_count = keep_mask.shape[1]
    masses = gathered[:, rows:].reshape(gathered.shape[0], -1).astype(jnp.float32)
    masses = sum(masses[:, k * block_count : (k + 1) * block_count] for k in range(3))
    here = block_count // device_count
    block_scores = lax.dynamic_slice_in_dim(masses, place * here, here, 1)
    return (cache_keys, cache_values, attended, block_scores)


def solution(mesh):
    placed = (
        P(("groups", "seq"), None, None),
        P(("groups", "seq"), None, None),
        P(("groups", "seq"), None, None, None),
        P("groups", None, None, None),
        P("groups", None, None),
        P("groups", None, None),
        P("groups"),
        P("groups", None),
    )
    return jax.shard_map(
        local,
        mesh=mesh,
        in_specs=placed,
        out_specs=(
            P("groups", "seq", None),
            P("groups", "seq", None),
            P("groups", None, None, None),
            P("groups", "seq"),
        ),
        check_vma=False,
    )
```
